8 devices in a mesh: tp: 4 (over z, y, x), cp: 2 (over core).
Axes of the slice: x: 2, y: 2, z: 1, core: 2. Of those that a mesh axis runs over, the one named last changes fastest.
Arguments:
- hidden: bfloat16 [3, 1024, 5120], P(None, 'cp')
- grad_out: bfloat16 [3, 1024, 5120], P(None, 'cp')
- w_dq: bfloat16 [5120, 1536], replicated
- g_q: bfloat16 [1536], replicated
- w_dkv: bfloat16 [5120, 576], replicated
- g_kv: bfloat16 [512], replicated
- w_uq: bfloat16 [1536, 128, 192], P(None, 'tp')
- w_uk: bfloat16 [512, 128, 128], P(None, 'tp')
- w_uv: bfloat16 [512, 128, 128], P(None, 'tp')
- w_o: bfloat16 [128, 128, 5120], P('tp')
Outputs:
- output 1: bfloat16 [3, 1024, 5120], P(None, 'cp')
- output 2: bfloat16 [3, 1024, 5120], P(None, 'cp')
- output 3: float32 [5120, 1536], replicated
- output 4: float32 [1536], replicated
- output 5: float32 [5120, 576], replicated
- output 6: float32 [512], replicated
- output 7: float32 [1536, 128, 192], P(None, 'tp')
- output 8: float32 [512, 128, 128], P(None, 'tp')
- output 9: float32 [512, 128, 128], P(None, 'tp')
- output 10: float32 [128, 128, 5120], P('tp')
All inputs are finite; a program needn't handle non-finite values.
Results may differ from the reference program's by a relative error of at most 0.014927.
Values are sent between devices in bfloat16 or wider.
A program may use at most 1.25 GiB of HBM per device.

```python
import jax
import jax.numpy as jnp
from jax import lax

D = 5120
HEADS = 128
Q_LORA = 1536
KV_LORA = 512
NOPE = 128
ROPE = 64
VHEAD = 128
BATCH = 3
SEQ_DEV = 512
CP = 2
QBLK = 64
THETA = 10000

SEQ = CP * SEQ_DEV
HALF_LEN = SEQ_DEV // 2
QK_DIM = NOPE + ROPE
EPS = 1e-6
NEG_BIG = -1e30


def token_positions():
    token_idx = jnp.arange(SEQ, dtype=jnp.int32)
    cp_rank = token_idx // SEQ_DEV
    local_idx = token_idx % SEQ_DEV
    block_id = jnp.where(local_idx < HALF_LEN, cp_rank, 2 * CP - 1 - cp_rank)
    return block_id * HALF_LEN + local_idx % HALF_LEN


def rope_tables(positions):
    inv_freq = 1.0 / (THETA ** (jnp.arange(ROPE // 2, dtype=jnp.float32) * 2.0 / ROPE))
    angles = positions.astype(jnp.float32)[:, None] * inv_freq[None, :]
    return jnp.cos(angles), jnp.sin(angles)


def apply_rope(values, cos_tab, sin_tab):
    half_dim = values.shape[-1] // 2
    lead_half = values[..., :half_dim]
    tail_half = values[..., half_dim:]
    return jnp.concatenate([lead_half * cos_tab - tail_half * sin_tab, tail_half * cos_tab + lead_half * sin_tab], axis=-1)


def rms_norm(raw_vals, gain_vec):
    raw_f32 = raw_vals.astype(jnp.float32)
    inv_rms = lax.rsqrt(jnp.mean(raw_f32 * raw_f32, axis=-1, keepdims=True) + EPS)
    return (raw_f32 * inv_rms * gain_vec).astype(jnp.bfloat16)


def attention(q_nope, q_pe, k_nope, k_pe, v_heads, positions):
    kn_f32 = k_nope.astype(jnp.float32)
    kp_f32 = k_pe.astype(jnp.float32)
    v_f32 = v_heads.astype(jnp.float32)
    n_blocks = SEQ // QBLK
    qn_blocks = jnp.moveaxis(q_nope.reshape(BATCH, n_blocks, QBLK, HEADS, NOPE), 1, 0)
    qp_blocks = jnp.moveaxis(q_pe.reshape(BATCH, n_blocks, QBLK, HEADS, ROPE), 1, 0)
    pos_blocks = positions.reshape(n_blocks, QBLK)

    def one_block(block_args):
        qn_blk, qp_blk, q_pos = block_args
        scores = jnp.einsum('bqhn,bkhn->bhqk', qn_blk.astype(jnp.float32), kn_f32) + jnp.einsum('bqhr,bkr->bhqk', qp_blk.astype(jnp.float32), kp_f32)
        scores = jnp.where(positions[None, :] <= q_pos[:, None], scores * QK_DIM ** -0.5, NEG_BIG)
        weights = jax.nn.softmax(scores, axis=-1)
        return jnp.einsum('bhqk,bkhv->bqhv', weights, v_f32).astype(jnp.bfloat16)

    out_blocks = lax.map(jax.checkpoint(one_block), (qn_blocks, qp_blocks, pos_blocks))
    return jnp.moveaxis(out_blocks, 0, 1).reshape(BATCH, SEQ, HEADS, VHEAD)


def forward(hidden, w_dq, g_q, w_dkv, g_kv, w_uq, w_uk, w_uv, w_o):
    positions = token_positions()
    cos_tab, sin_tab = rope_tables(positions)
    hidden_f32 = hidden.astype(jnp.float32)
    cq_raw = jnp.einsum('btd,dq->btq', hidden_f32, w_dq).astype(jnp.bfloat16)
    kv_raw = jnp.einsum('btd,dc->btc', hidden_f32, w_dkv).astype(jnp.bfloat16)
    c_q = rms_norm(cq_raw, g_q)
    c_kv = rms_norm(kv_raw[..., :KV_LORA], g_kv)
    k_pe = apply_rope(kv_raw[..., KV_LORA:].astype(jnp.float32), cos_tab, sin_tab).astype(jnp.bfloat16)
    q_all = jnp.einsum('btq,qhe->bthe', c_q.astype(jnp.float32), w_uq).astype(jnp.bfloat16)
    q_nope = q_all[..., :NOPE]
    q_pe = apply_rope(q_all[..., NOPE:].astype(jnp.float32), cos_tab[:, None, :], sin_tab[:, None, :]).astype(jnp.bfloat16)
    k_nope = jnp.einsum('btc,chn->bthn', c_kv.astype(jnp.float32), w_uk).astype(jnp.bfloat16)
    v_heads = jnp.einsum('btc,chv->bthv', c_kv.astype(jnp.float32), w_uv).astype(jnp.bfloat16)
    o_heads = attention(q_nope, q_pe, k_nope, k_pe, v_heads, positions)
    return jnp.einsum('bthv,hvd->btd', o_heads.astype(jnp.float32), w_o).astype(jnp.bfloat16)


def setup_inputs(seed: int = 0) -> dict:
    rng_keys = jax.random.split(jax.random.key(seed), 10)

    def normal_weight(rng_key, arr_shape, fan_in):
        return (jax.random.normal(rng_key, arr_shape, jnp.float32) * fan_in ** -0.5).astype(jnp.bfloat16)

    return {
        'hidden': jax.random.normal(rng_keys[0], (BATCH, SEQ, D), jnp.float32).astype(jnp.bfloat16),
        'grad_out': jax.random.normal(rng_keys[1], (BATCH, SEQ, D), jnp.float32).astype(jnp.bfloat16),
        'w_dq': normal_weight(rng_keys[2], (D, Q_LORA), D),
        'g_q': jax.random.uniform(rng_keys[3], (Q_LORA,), jnp.float32, 0.5, 1.5).astype(jnp.bfloat16),
        'w_dkv': normal_weight(rng_keys[4], (D, KV_LORA + ROPE), D),
        'g_kv': jax.random.uniform(rng_keys[5], (KV_LORA,), jnp.float32, 0.5, 1.5).astype(jnp.bfloat16),
        'w_uq': normal_weight(rng_keys[6], (Q_LORA, HEADS, QK_DIM), Q_LORA),
        'w_uk': normal_weight(rng_keys[7], (KV_LORA, HEADS, NOPE), KV_LORA),
        'w_uv': normal_weight(rng_keys[8], (KV_LORA, HEADS, VHEAD), KV_LORA),
        'w_o': normal_weight(rng_keys[9], (HEADS, VHEAD, D), HEADS * VHEAD),
    }


def reference(hidden, grad_out, w_dq, g_q, w_dkv, g_kv, w_uq, w_uk, w_uv, w_o):
    attn_out, pullback = jax.vjp(forward, hidden, w_dq.astype(jnp.float32), g_q.astype(jnp.float32), w_dkv.astype(jnp.float32), g_kv.astype(jnp.float32), w_uq.astype(jnp.float32), w_uk.astype(jnp.float32), w_uv.astype(jnp.float32), w_o.astype(jnp.float32))
    all_grads = pullback(grad_out)
    return (attn_out, all_grads[0], all_grads[1], all_grads[2], all_grads[3], all_grads[4], all_grads[5], all_grads[6], all_grads[7], all_grads[8])
```

```python
import functools

import jax
import jax.numpy as jnp
from jax import lax
from jax.experimental import pallas as pl
from jax.experimental.pallas import tpu as pltpu
from jax.sharding import PartitionSpec as P

EPS = 1e-6
THETA = 10000.0
NEG_BIG = -1e30
LOG2E = 1.4426950408889634
BLOCK_SLOT = (0, 1, 1, 0)
BLOCK_HALF = (0, 0, 1, 1)
F32 = jnp.float32
BF16 = jnp.bfloat16


def layout_positions(seq_local, cp_size, cp_rank):
    half_len = seq_local // 2
    local_idx = jnp.arange(seq_local, dtype=jnp.int32)
    block_id = jnp.where(local_idx < half_len, cp_rank, 2 * cp_size - 1 - cp_rank)
    return block_id * half_len + local_idx % half_len


def rope_tables(positions, rope_dim):
    inv_freq = 1.0 / (THETA ** (jnp.arange(rope_dim // 2, dtype=F32) * 2.0 / rope_dim))
    angles = positions.astype(F32)[:, None] * inv_freq[None, :]
    return jnp.cos(angles), jnp.sin(angles)


def apply_rope(values, cos_tab, sin_tab):
    half_dim = values.shape[-1] // 2
    lead_half = values[..., :half_dim]
    tail_half = values[..., half_dim:]
    return jnp.concatenate([lead_half * cos_tab - tail_half * sin_tab, tail_half * cos_tab + lead_half * sin_tab], axis=-1)


def unrope(grad_vals, cos_tab, sin_tab):
    half_dim = grad_vals.shape[-1] // 2
    lead_half = grad_vals[..., :half_dim]
    tail_half = grad_vals[..., half_dim:]
    return jnp.concatenate([lead_half * cos_tab + tail_half * sin_tab, tail_half * cos_tab - lead_half * sin_tab], axis=-1)


def norm_f32(raw_vals, gain_vec):
    inv_rms = lax.rsqrt(jnp.mean(raw_vals * raw_vals, axis=-1, keepdims=True) + EPS)
    return raw_vals * inv_rms * gain_vec


def dot(lhs, rhs, lhs_dim, rhs_dim):
    return lax.dot_general(lhs, rhs, (((lhs_dim,), (rhs_dim,)), ((), ())), preferred_element_type=F32)


def attn_kernel(scale, n_alias, rank_ref, q_ref, k_ref, v_ref, kp_ref, do0_ref, do1_ref, cos_ref, sin_ref, *rest):
    o_now_ref, o_ref, dq_ref, dk_ref, dv_ref, dkp_ref, kcat, vcat, qcat, dk_acc, dv_acc = rest[n_alias:]
    rank = rank_ref[0]
    blk = q_ref.shape[4] // 2
    nope = k_ref.shape[3]
    qk = q_ref.shape[3]
    half = (qk - nope) // 2
    mid = nope + half

    def where_is(p):
        return jnp.bitwise_xor(rank, BLOCK_SLOT[p]), slice(BLOCK_HALF[p] * blk, BLOCK_HALF[p] * blk + blk)

    for p in range(4):
        slot, rows = where_is(p)
        dst = slice(p * blk, p * blk + blk)
        kcat[dst, :nope] = k_ref[slot, 0, rows, :]
        kcat[dst, nope:] = kp_ref[slot, 0, rows, :]
        vcat[dst, :] = v_ref[slot, 0, rows, :]

    for p in (3, 2, 1, 0):
        slot, rows = where_is(p)
        n_keys = (p + 1) * blk
        cos_p = cos_ref[:, p * blk:p * blk + blk]
        sin_p = sin_ref[:, p * blk:p * blk + blk]
        lead = q_ref[0, slot, 0, nope:mid, rows].astype(F32)
        tail = q_ref[0, slot, 0, mid:, rows].astype(F32)
        qcat[p, :nope, :] = q_ref[0, slot, 0, :nope, rows]
        qcat[p, nope:mid, :] = (lead * cos_p - tail * sin_p).astype(BF16)
        qcat[p, mid:, :] = (tail * cos_p + lead * sin_p).astype(BF16)
        q_blk = qcat[p]
        do_blk = jnp.where(slot == 0, do0_ref[0, 0, :, rows], do1_ref[0, 0, :, rows])
        keys = kcat[:n_keys, :]
        vals = vcat[:n_keys, :]
        st = dot(keys, q_blk, 1, 0)
        key_id = lax.broadcasted_iota(jnp.int32, (blk, blk), 0)
        qry_id = lax.broadcasted_iota(jnp.int32, (blk, blk), 1)
        diag = jnp.where(key_id <= qry_id, st[n_keys - blk:, :], NEG_BIG)
        st = diag if p == 0 else jnp.concatenate([st[:n_keys - blk, :], diag], axis=0)
        col_max = jnp.max(st, axis=0, keepdims=True)
        prob = jnp.exp2((st - col_max) * (scale * LOG2E))
        prob = prob * (1.0 / jnp.sum(prob, axis=0, keepdims=True))
        prob_b = prob.astype(BF16)
        out_blk = dot(vals, prob_b, 0, 0).astype(BF16)
        o_ref[slot, 0, 0, :, rows] = out_blk
        o_now_ref[slot, 0, :, rows] = out_blk
        dpt = dot(vals, do_blk, 1, 0)
        row_dot = jnp.sum(prob * dpt, axis=0, keepdims=True)
        dst_b = (prob * (dpt - row_dot)).astype(BF16)
        dq = dot(keys, dst_b, 0, 0) * scale
        lead = dq[nope:mid, :]
        tail = dq[mid:, :]
        dq_ref[slot, 0, 0, :nope, rows] = dq[:nope, :].astype(BF16)
        dq_ref[slot, 0, 0, nope:mid, rows] = (lead * cos_p + tail * sin_p).astype(BF16)
        dq_ref[slot, 0, 0, mid:, rows] = (tail * cos_p - lead * sin_p).astype(BF16)
        dk_part = dot(dst_b, q_blk, 1, 1)
        dv_part = dot(prob_b, do_blk, 1, 1)
        if p == 3:
            dk_acc[...] = dk_part
            dv_acc[...] = dv_part
        else:
            dk_acc[:n_keys, :] += dk_part
            dv_acc[:n_keys, :] += dv_part

    @pl.when(pl.program_id(0) == 0)
    def _():
        dkp_ref[...] = jnp.zeros_like(dkp_ref)

    for p in range(4):
        slot, rows = where_is(p)
        src = slice(p * blk, p * blk + blk)
        dk_ref[slot, 0, rows, :] = (dk_acc[src, :nope] * scale).astype(BF16)
        dv_ref[slot, 0, rows, :] = dv_acc[src, :].astype(BF16)
        dkp_ref[slot, rows, :] += dk_acc[src, nope:] * scale


def attention(batch, rank, q, k, v, kp, do0, do1, cos_t, sin_t, chain):
    heads, _, n_batch, qk, seq = q.shape
    v_dim = do0.shape[2]
    rope = kp.shape[3]
    nope = qk - rope

    def whole(*shape):
        return pl.BlockSpec(shape, lambda h, r: (0,) * len(shape))

    q_spec = pl.BlockSpec((1, 2, 1, qk, seq), lambda h, r: (h, 0, batch, 0, 0))
    k_spec = pl.BlockSpec((2, 1, seq, nope), lambda h, r: (0, batch, 0, h))
    v_spec = pl.BlockSpec((2, 1, seq, v_dim), lambda h, r: (0, batch, 0, h))
    do_spec = pl.BlockSpec((1, 1, v_dim, seq), lambda h, r: (h, batch, 0, 0))
    o_spec = pl.BlockSpec((2, 1, 1, v_dim, seq), lambda h, r: (0, h, batch, 0, 0))
    dq_spec = pl.BlockSpec((2, 1, 1, qk, seq), lambda h, r: (0, h, batch, 0, 0))
    shared = [jax.ShapeDtypeStruct((2, heads, n_batch, v_dim, seq), BF16), jax.ShapeDtypeStruct((2, heads, n_batch, qk, seq), BF16),
              jax.ShapeDtypeStruct(k.shape, BF16), jax.ShapeDtypeStruct(v.shape, BF16)]
    n_alias = len(chain)
    n_scores = heads * (4 * seq * seq) * 5 // 8
    return pl.pallas_call(
        functools.partial(attn_kernel, qk ** -0.5, n_alias),
        out_shape=[jax.ShapeDtypeStruct((2, heads, v_dim, seq), BF16)] + shared + [jax.ShapeDtypeStruct((2, seq, rope), F32)],
        grid_spec=pltpu.PrefetchScalarGridSpec(
            num_scalar_prefetch=1,
            grid=(heads,),
            in_specs=[q_spec, k_spec, v_spec, pl.BlockSpec((2, 1, seq, rope), lambda h, r: (0, batch, 0, 0)),
                      do_spec, do_spec, whole(rope // 2, 2 * seq), whole(rope // 2, 2 * seq)]
            + [pl.BlockSpec(memory_space=pl.ANY)] * n_alias,
            out_specs=[pl.BlockSpec((2, 1, v_dim, seq), lambda h, r: (0, h, 0, 0)),
                       o_spec, dq_spec, k_spec, v_spec, whole(2, seq, rope)],
            scratch_shapes=[pltpu.VMEM((2 * seq, qk), BF16), pltpu.VMEM((2 * seq, v_dim), BF16),
                            pltpu.VMEM((4, qk, seq // 2), BF16),
                            pltpu.VMEM((2 * seq, qk), F32), pltpu.VMEM((2 * seq, v_dim), F32)],
        ),
        input_output_aliases={9 + i: 1 + i for i in range(n_alias)},
        compiler_params=pltpu.CompilerParams(dimension_semantics=("arbitrary",), vmem_limit_bytes=40 * 2 ** 20),
        cost_estimate=pl.CostEstimate(flops=5 * n_scores * (qk + v_dim), bytes_accessed=heads * seq * 16 * 256, transcendentals=n_scores),
        name="attn_fwd_bwd",
    )(rank, q, k, v, kp, do0, do1, cos_t, sin_t, *chain)


def merge_kernel(rank_ref, mine_ref, other_ref, out_ref):
    is_mine = pl.program_id(0) == rank_ref[0]

    @pl.when(is_mine)
    def _():
        out_ref[...] = mine_ref[...]

    @pl.when(jnp.logical_not(is_mine))
    def _():
        out_ref[...] = other_ref[...]


def merge_halves(rank, mine, other, axis, tile):
    lead, mid, width = mine.shape
    if axis == 0:
        block, steps = (tile, mid, width), lead // tile
        out_map = lambda half, i, r: (half * steps + i, 0, 0)
        out_shape = (2 * lead, mid, width)
    else:
        block, steps = (tile, mid, width), lead // tile
        out_map = lambda half, i, r: (i, half, 0)
        out_shape = (lead, 2 * mid, width)
    last = steps - 1
    mine_map = lambda half, i, r: (jnp.where(half == r[0], i, jnp.where(half == 0, 0, last)), 0, 0)
    other_map = lambda half, i, r: (jnp.where(half != r[0], i, jnp.where(half == 0, 0, last)), 0, 0)
    n_bytes = 4 * mine.size * 4
    return pl.pallas_call(
        merge_kernel,
        out_shape=jax.ShapeDtypeStruct(out_shape, mine.dtype),
        grid_spec=pltpu.PrefetchScalarGridSpec(
            num_scalar_prefetch=1, grid=(2, steps),
            in_specs=[pl.BlockSpec(block, mine_map), pl.BlockSpec(block, other_map)],
            out_specs=pl.BlockSpec(block, out_map)),
        compiler_params=pltpu.CompilerParams(dimension_semantics=("arbitrary", "arbitrary"), vmem_limit_bytes=48 * 2 ** 20),
        cost_estimate=pl.CostEstimate(flops=n_bytes * 100, bytes_accessed=n_bytes, transcendentals=0),
        name="merge_halves",
    )(rank, mine, other)


def down_wgrad_kernel(x0_ref, x1_ref, q0_ref, q1_ref, c0_ref, c1_ref, dq_ref, dc_ref):
    x0 = x0_ref[...]
    x1 = x1_ref[...]
    dq_ref[...] = dot(x0, q0_ref[...], 0, 0) + dot(x1, q1_ref[...], 0, 0)
    dc_ref[...] = dot(c0_ref[...], x0, 0, 0) + dot(c1_ref[...], x1, 0, 0)


def down_wgrad(x0, x1, q0, q1, c0, c1):
    width, q_dim, c_dim = x0.shape[-1], q0.shape[-1], c0.shape[-1]
    operands = [value.reshape(-1, value.shape[-1]) for value in (x0, x1, q0, q1, c0, c1)]
    tokens = operands[0].shape[0]
    tile = min(width, 256)
    x_spec = pl.BlockSpec((tokens, tile), lambda i: (0, i))
    q_spec = pl.BlockSpec((tokens, q_dim), lambda i: (0, 0))
    c_spec = pl.BlockSpec((tokens, c_dim), lambda i: (0, 0))
    grad_q, grad_c = pl.pallas_call(
        down_wgrad_kernel,
        out_shape=[jax.ShapeDtypeStruct((width, q_dim), F32), jax.ShapeDtypeStruct((c_dim, width), F32)],
        grid=(width // tile,),
        in_specs=[x_spec, x_spec, q_spec, q_spec, c_spec, c_spec],
        out_specs=[pl.BlockSpec((tile, q_dim), lambda i: (i, 0)), pl.BlockSpec((c_dim, tile), lambda i: (0, i))],
        compiler_params=pltpu.CompilerParams(dimension_semantics=("arbitrary",), vmem_limit_bytes=56 * 2 ** 20),
        cost_estimate=pl.CostEstimate(flops=4 * tokens * width * (q_dim + c_dim), bytes_accessed=4 * tokens * width + 4 * width * (q_dim + c_dim), transcendentals=0),
        name="down_wgrad",
    )(*operands)
    return grad_q, grad_c.T


def solution(mesh):
    cp_size = mesh.shape['cp']
    tp_size = mesh.shape['tp']
    swap_pairs = [(0, 1), (1, 0)]

    def swap(value):
        return lax.ppermute(value, 'cp', swap_pairs)

    def with_other(value):
        return jnp.stack([value, swap(value)])

    def per_device(hidden, grad_out, w_dq, g_q, w_dkv, g_kv, w_uq, w_uk, w_uv, w_o):
        cp_rank = lax.axis_index('cp')
        tp_rank = lax.axis_index('tp')
        rank = cp_rank.astype(jnp.int32)[None]
        n_batch, seq_local, _ = hidden.shape
        q_lora = w_dq.shape[1]
        kv_lora = g_kv.shape[0]
        nope_dim = w_uk.shape[2]
        v_dim = w_uv.shape[2]
        qk_dim = w_uq.shape[2]
        rope_dim = qk_dim - nope_dim
        heads_core = w_uq.shape[1] // cp_size
        tok_tp = seq_local // tp_size

        positions = layout_positions(seq_local, cp_size, cp_rank)
        cos_tab, sin_tab = rope_tables(positions, rope_dim)
        cos_nat, sin_nat = rope_tables(jnp.arange(cp_size * seq_local, dtype=jnp.int32), rope_dim)
        cos_t, sin_t = cos_nat.T, sin_nat.T

        head0 = cp_rank * heads_core
        uq_mine = lax.dynamic_slice_in_dim(jnp.transpose(w_uq, (1, 2, 0)), head0, heads_core, 0)
        uk_mine = lax.dynamic_slice_in_dim(w_uk, head0, heads_core, 1).reshape(kv_lora, heads_core * nope_dim)
        uv_mine = lax.dynamic_slice_in_dim(w_uv, head0, heads_core, 1).reshape(kv_lora, heads_core * v_dim)
        wo_mine = lax.dynamic_slice_in_dim(w_o, head0, heads_core, 0)

        cq_raw = jnp.einsum('btd,dq->btq', hidden, w_dq, preferred_element_type=F32).astype(BF16)
        kv_raw = jnp.einsum('btd,dc->btc', hidden, w_dkv, preferred_element_type=F32).astype(BF16)
        gq_f32 = g_q.astype(F32)
        gkv_f32 = g_kv.astype(F32)
        c_q = norm_f32(cq_raw.astype(F32), gq_f32).astype(BF16)
        c_kv = norm_f32(kv_raw[..., :kv_lora].astype(F32), gkv_f32).astype(BF16)
        k_pe = apply_rope(kv_raw[..., kv_lora:].astype(F32), cos_tab, sin_tab).astype(BF16)

        c_q2 = with_other(c_q)
        c_kv2 = with_other(c_kv)
        k_pe2 = with_other(k_pe)
        dy_other = swap(grad_out)

        def head_grads(dy):
            return jnp.einsum('hvd,btd->hbvt', wo_mine, dy, preferred_element_type=F32).astype(BF16)

        do0 = head_grads(grad_out)
        do1 = head_grads(dy_other)
        q_all = jnp.einsum('heq,sbtq->hsbet', uq_mine, c_q2, preferred_element_type=F32).astype(BF16)
        k_nope = jnp.einsum('sbtc,cn->sbtn', c_kv2, uk_mine, preferred_element_type=F32).astype(BF16)
        v_heads = jnp.einsum('sbtc,cv->sbtv', c_kv2, uv_mine, preferred_element_type=F32).astype(BF16)

        x_late, q_all = lax.optimization_barrier((hidden, q_all))
        x_other = swap(x_late)

        chain = ()
        dkp_parts = []
        y_parts = []
        for b in range(n_batch):
            res = attention(b, rank, q_all, k_nope, v_heads, k_pe2, do0, do1, cos_t, sin_t, chain)
            o_now, chain, dkp = res[0], tuple(res[1:5]), res[5]
            dkp_parts.append(dkp)
            o_recv = swap(o_now[1])
            o_full = jnp.concatenate([jnp.where(cp_rank == 0, o_now[0], o_recv), jnp.where(cp_rank == 0, o_recv, o_now[0])], axis=0)
            y_b = jnp.einsum('hvt,hvd->td', o_full, w_o, preferred_element_type=F32)
            chain, y_b = lax.optimization_barrier((chain, y_b))
            y_parts.append(lax.psum_scatter(y_b, 'tp', scatter_dimension=0, tiled=True).astype(BF16))
        o_all, dq_all, dk_all, dv_all = chain

        def latent_grads(slot):
            dcq = jnp.einsum('hbet,heq->btq', dq_all[slot], uq_mine, preferred_element_type=F32)
            dckv = jnp.einsum('btn,cn->btc', dk_all[slot], uk_mine, preferred_element_type=F32) + jnp.einsum('btv,cv->btc', dv_all[slot], uv_mine, preferred_element_type=F32)
            return dcq, dckv

        dcq_away, dckv_away = latent_grads(1)
        dcq_home, dckv_home = latent_grads(0)
        dkp2 = jnp.stack(dkp_parts, axis=1)
        latent_part = jnp.concatenate([
            dcq_home + swap(dcq_away),
            dckv_home + swap(dckv_away),
            dkp2[0] + swap(dkp2[1])], axis=-1)
        latent_part, y_parts = lax.optimization_barrier((latent_part, y_parts))
        latent_grad = lax.psum_scatter(latent_part, 'tp', scatter_dimension=1, tiled=True)

        def my_tokens(value, axis):
            return lax.dynamic_slice_in_dim(value, tp_rank * tok_tp, tok_tp, axis)

        cq_mine = my_tokens(cq_raw, 1).astype(F32)
        ckv_mine = my_tokens(kv_raw, 1)[..., :kv_lora].astype(F32)
        grad_cq_raw, grad_g_q = jax.vjp(norm_f32, cq_mine, gq_f32)[1](latent_grad[..., :q_lora])
        grad_ckv_raw, grad_g_kv = jax.vjp(norm_f32, ckv_mine, gkv_f32)[1](latent_grad[..., q_lora:q_lora + kv_lora])
        grad_kpe_raw = unrope(latent_grad[..., q_lora + kv_lora:], my_tokens(cos_tab, 0), my_tokens(sin_tab, 0))
        draw = jnp.concatenate([grad_cq_raw, grad_ckv_raw, grad_kpe_raw], axis=-1).astype(BF16)
        draw = lax.all_gather(draw, 'tp', axis=1, tiled=True)
        grad_g_q, grad_g_kv = lax.psum((grad_g_q, grad_g_kv), ('tp', 'cp'))

        y_stack, draw = lax.optimization_barrier((jnp.stack(y_parts), draw))
        attn_out = lax.all_gather(y_stack, 'tp', axis=1, tiled=True)

        grad_w_o = jnp.einsum('hbvt,btd->hvd', o_all[0], grad_out, preferred_element_type=F32) + jnp.einsum('hbvt,btd->hvd', o_all[1], dy_other, preferred_element_type=F32)
        grad_w_uq = jnp.einsum('shbet,sbtq->heq', dq_all, c_q2, preferred_element_type=F32)
        grad_w_uk = jnp.einsum('sbtc,sbtn->cn', c_kv2, dk_all, preferred_element_type=F32).reshape(kv_lora, heads_core, nope_dim)
        grad_w_uv = jnp.einsum('sbtc,sbtv->cv', c_kv2, dv_all, preferred_element_type=F32).reshape(kv_lora, heads_core, v_dim)
        grad_w_o = merge_halves(rank, grad_w_o, swap(grad_w_o), 0, 1)
        grad_w_uq = jnp.transpose(merge_halves(rank, grad_w_uq, swap(grad_w_uq), 0, 2), (2, 0, 1))
        grad_w_uk = merge_halves(rank, grad_w_uk, swap(grad_w_uk), 1, min(kv_lora, 256))
        grad_w_uv = merge_halves(rank, grad_w_uv, swap(grad_w_uv), 1, min(kv_lora, 256))

        dcq_raw, dkv_raw = lax.optimization_barrier((draw[..., :q_lora], draw[..., q_lora:]))
        dcq_other, dkv_other = swap(dcq_raw), swap(dkv_raw)
        grad_hidden = (jnp.einsum('btq,dq->btd', dcq_raw, w_dq, preferred_element_type=F32) + jnp.einsum('btc,dc->btd', dkv_raw, w_dkv, preferred_element_type=F32)).astype(BF16)
        grad_w_dq, grad_w_dkv = down_wgrad(hidden, x_other, dcq_raw, dcq_other, dkv_raw, dkv_other)
        return (attn_out, grad_hidden, grad_w_dq, grad_g_q, grad_w_dkv, grad_g_kv, grad_w_uq, grad_w_uk, grad_w_uv, grad_w_o)

    seq_spec = P(None, 'cp', None)
    full_spec = P()
    head_spec = P(None, 'tp', None)
    out_head_spec = P('tp', None, None)
    all_specs = (seq_spec, seq_spec, full_spec, full_spec, full_spec, full_spec, head_spec, head_spec, head_spec, out_head_spec)
    return jax.shard_map(per_device, mesh=mesh, in_specs=all_specs, out_specs=all_specs, check_vma=False)
```

```python
import functools

import jax
import jax.numpy as jnp
from jax import lax
from jax.experimental import pallas as pl
from jax.experimental.pallas import tpu as pltpu
from jax.sharding import PartitionSpec as P


EPS = 1e-6
THETA = 10000.0
NEG_BIG = -1e30
LOG2E = 1.4426950408889634
BLOCK_SLOT = (0, 1, 1, 0)
BLOCK_HALF = (0, 0, 1, 1)
F32 = jnp.float32
BF16 = jnp.bfloat16


def layout_positions(seq_local, cp_size, cp_rank):
    half_len = seq_local // 2
    local_idx = jnp.arange(seq_local, dtype=jnp.int32)
    block_id = jnp.where(local_idx < half_len, cp_rank, 2 * cp_size - 1 - cp_rank)
    return block_id * half_len + local_idx % half_len


def rope_tables(positions, rope_dim):
    inv_freq = 1.0 / (THETA ** (jnp.arange(rope_dim // 2, dtype=F32) * 2.0 / rope_dim))
    angles = positions.astype(F32)[:, None] * inv_freq[None, :]
    return jnp.cos(angles), jnp.sin(angles)


def apply_rope(values, cos_tab, sin_tab):
    half_dim = values.shape[-1] // 2
    lead_half = values[..., :half_dim]
    tail_half = values[..., half_dim:]
    return jnp.concatenate([lead_half * cos_tab - tail_half * sin_tab, tail_half * cos_tab + lead_half * sin_tab], axis=-1)


def unrope(grad_vals, cos_tab, sin_tab):
    half_dim = grad_vals.shape[-1] // 2
    lead_half = grad_vals[..., :half_dim]
    tail_half = grad_vals[..., half_dim:]
    return jnp.concatenate([lead_half * cos_tab + tail_half * sin_tab, tail_half * cos_tab - lead_half * sin_tab], axis=-1)


def norm_f32(raw_vals, gain_vec):
    inv_rms = lax.rsqrt(jnp.mean(raw_vals * raw_vals, axis=-1, keepdims=True) + EPS)
    return raw_vals * inv_rms * gain_vec


def dot(lhs, rhs, lhs_dim, rhs_dim):
    return lax.dot_general(lhs, rhs, (((lhs_dim,), (rhs_dim,)), ((), ())), preferred_element_type=F32)


def attn_kernel(scale, n_alias, rank_ref, q_ref, k_ref, v_ref, kp_ref, do0_ref, do1_ref, cos_ref, sin_ref, *rest):
    o_now_ref, o_ref, dq_ref, dk_ref, dv_ref, dkp_ref, kcat, k_t, v_t, qcat, dk_acc, dv_acc, score, prob_b, grad_s = rest[n_alias:]
    rank = rank_ref[0]
    blk = q_ref.shape[4] // 2
    nope = k_ref.shape[3]
    qk = q_ref.shape[3]
    half = (qk - nope) // 2
    mid = nope + half
    place = [(jnp.bitwise_xor(rank, BLOCK_SLOT[p]), slice(BLOCK_HALF[p] * blk, BLOCK_HALF[p] * blk + blk)) for p in range(4)]

    def span(p):
        return slice(p * blk, p * blk + blk)

    @pl.when(pl.program_id(0) == 0)
    def _():
        dkp_ref[...] = jnp.zeros_like(dkp_ref)
        for p in range(4):
            slot, rows = place[p]
            k_rope = kp_ref[slot, 0, rows, :]
            kcat[span(p), nope:] = k_rope
            k_t[nope:, span(p)] = k_rope.T

    for p in range(4):
        slot, rows = place[p]
        k_blk = k_ref[slot, 0, rows, :]
        kcat[span(p), :nope] = k_blk
        k_t[:nope, span(p)] = k_blk.T
        v_t[:, span(p)] = v_ref[slot, 0, rows, :].T

    untouched = [True] * 4
    pending = [4 - j for j in range(4)]

    def flush(j):
        slot, rows = place[j]
        dk_ref[slot, 0, rows, :] = (dk_acc[span(j), :nope] * scale).astype(BF16)
        dv_ref[slot, 0, rows, :] = dv_acc[span(j), :].astype(BF16)
        dkp_ref[slot, rows, :] += dk_acc[span(j), nope:] * scale

    def steps(p, buf):
        slot, rows = place[p]
        n_blk = p + 1
        yield False, 0
        cos_p = cos_ref[:, span(p)]
        sin_p = sin_ref[:, span(p)]
        lead = q_ref[0, slot, 0, nope:mid, rows].astype(F32)
        tail = q_ref[0, slot, 0, mid:, rows].astype(F32)
        qcat[p, :nope, :] = q_ref[0, slot, 0, :nope, rows]
        qcat[p, nope:mid, :] = (lead * cos_p - tail * sin_p).astype(BF16)
        qcat[p, mid:, :] = (tail * cos_p + lead * sin_p).astype(BF16)
        col_max = None
        for j in range(n_blk):
            yield True, 2
            st = dot(kcat[span(j), :], qcat[p], 1, 0)
            if j == p:
                key_id = lax.broadcasted_iota(jnp.int32, (blk, blk), 0)
                qry_id = lax.broadcasted_iota(jnp.int32, (blk, blk), 1)
                st = jnp.where(key_id <= qry_id, st, NEG_BIG)
            score[buf, span(j), :] = st
            part = jnp.max(st, axis=0, keepdims=True)
            col_max = part if col_max is None else jnp.maximum(col_max, part)
        col_sum = None
        for j in range(n_blk):
            yield False, 3
            prob = jnp.exp2((score[buf, span(j), :] - col_max) * (scale * LOG2E))
            score[buf, span(j), :] = prob
            part = jnp.sum(prob, axis=0, keepdims=True)
            col_sum = part if col_sum is None else col_sum + part
        inv_sum = 1.0 / col_sum
        for j in range(n_blk):
            yield False, 2
            prob_b[buf, span(j), :] = (score[buf, span(j), :] * inv_sum).astype(BF16)
        n_keys = n_blk * blk
        yield True, n_blk
        out = dot(v_t[:, :n_keys], prob_b[buf, :n_keys, :], 1, 0)
        out_b = out.astype(BF16)
        o_ref[slot, 0, 0, :, rows] = out_b
        o_now_ref[slot, 0, :, rows] = out_b
        do_blk = jnp.where(slot == 0, do0_ref[0, 0, :, rows], do1_ref[0, 0, :, rows])
        row_dot = jnp.sum(out * do_blk.astype(F32), axis=0, keepdims=True)
        for j in range(n_blk):
            yield True, 2
            v_slot, v_rows = place[j]
            dprob = dot(v_ref[v_slot, 0, v_rows, :], do_blk, 1, 0)
            grad_s[buf, span(j), :] = (score[buf, span(j), :] * ((dprob - row_dot) * inv_sum)).astype(BF16)
        for j in range(n_blk):
            yield True, 4
            dk_part = dot(grad_s[buf, span(j), :], qcat[p], 1, 1)
            dv_part = dot(prob_b[buf, span(j), :], do_blk, 1, 1)
            if untouched[j]:
                dk_acc[span(j), :] = dk_part
                dv_acc[span(j), :] = dv_part
                untouched[j] = False
            else:
                dk_acc[span(j), :] += dk_part
                dv_acc[span(j), :] += dv_part
            pending[j] -= 1
            if pending[j] == 0:
                flush(j)
        yield True, n_blk
        dq = dot(k_t[:, :n_keys], grad_s[buf, :n_keys, :], 1, 0) * scale
        lead = dq[nope:mid, :]
        tail = dq[mid:, :]
        dq_ref[slot, 0, 0, :nope, rows] = dq[:nope, :].astype(BF16)
        dq_ref[slot, 0, 0, nope:mid, rows] = (lead * cos_p + tail * sin_p).astype(BF16)
        dq_ref[slot, 0, 0, mid:, rows] = (tail * cos_p - lead * sin_p).astype(BF16)

    def stream(blocks, buf):
        for p in blocks:
            yield from steps(p, buf)

    streams = [stream((3, 0), 0), stream((2, 1), 1)]
    heads_of = [next(st) for st in streams]
    busy = {True: 0, False: 0}
    while any(nxt is not None for nxt in heads_of):
        ready = [i for i in range(2) if heads_of[i] is not None]
        pick = min(ready, key=lambda i: (busy[heads_of[i][0]], i))
        is_mxu, cost = heads_of[pick]
        busy[is_mxu] += cost
        heads_of[pick] = next(streams[pick], None)


def attention(batch, rank, q, k, v, kp, do0, do1, cos_t, sin_t, chain):
    heads, _, n_batch, qk, seq = q.shape
    v_dim = do0.shape[2]
    rope = kp.shape[3]
    nope = qk - rope

    def whole(*shape):
        return pl.BlockSpec(shape, lambda h, r: (0,) * len(shape))

    q_spec = pl.BlockSpec((1, 2, 1, qk, seq), lambda h, r: (h, 0, batch, 0, 0))
    k_spec = pl.BlockSpec((2, 1, seq, nope), lambda h, r: (0, batch, 0, h))
    v_spec = pl.BlockSpec((2, 1, seq, v_dim), lambda h, r: (0, batch, 0, h))
    do_spec = pl.BlockSpec((1, 1, v_dim, seq), lambda h, r: (h, batch, 0, 0))
    o_spec = pl.BlockSpec((2, 1, 1, v_dim, seq), lambda h, r: (0, h, batch, 0, 0))
    dq_spec = pl.BlockSpec((2, 1, 1, qk, seq), lambda h, r: (0, h, batch, 0, 0))
    shared = [jax.ShapeDtypeStruct((2, heads, n_batch, v_dim, seq), BF16), jax.ShapeDtypeStruct((2, heads, n_batch, qk, seq), BF16),
              jax.ShapeDtypeStruct(k.shape, BF16), jax.ShapeDtypeStruct(v.shape, BF16)]
    n_alias = len(chain)
    n_scores = heads * (4 * seq * seq) * 5 // 8
    return pl.pallas_call(
        functools.partial(attn_kernel, qk ** -0.5, n_alias),
        out_shape=[jax.ShapeDtypeStruct((2, heads, v_dim, seq), BF16)] + shared + [jax.ShapeDtypeStruct((2, seq, rope), F32)],
        grid_spec=pltpu.PrefetchScalarGridSpec(
            num_scalar_prefetch=1,
            grid=(heads,),
            in_specs=[q_spec, k_spec, v_spec, pl.BlockSpec((2, 1, seq, rope), lambda h, r: (0, batch, 0, 0)),
                      do_spec, do_spec, whole(rope // 2, 2 * seq), whole(rope // 2, 2 * seq)]
            + [pl.BlockSpec(memory_space=pl.ANY)] * n_alias,
            out_specs=[pl.BlockSpec((2, 1, v_dim, seq), lambda h, r: (0, h, 0, 0)),
                       o_spec, dq_spec, k_spec, v_spec, whole(2, seq, rope)],
            scratch_shapes=[pltpu.VMEM((2 * seq, qk), BF16), pltpu.VMEM((qk, 2 * seq), BF16), pltpu.VMEM((v_dim, 2 * seq), BF16),
                            pltpu.VMEM((4, qk, seq // 2), BF16),
                            pltpu.VMEM((2 * seq, qk), F32), pltpu.VMEM((2 * seq, v_dim), F32),
                            pltpu.VMEM((2, 2 * seq, seq // 2), F32), pltpu.VMEM((2, 2 * seq, seq // 2), BF16),
                            pltpu.VMEM((2, 2 * seq, seq // 2), BF16)],
        ),
        input_output_aliases={9 + i: 1 + i for i in range(n_alias)},
        compiler_params=pltpu.CompilerParams(dimension_semantics=("arbitrary",), vmem_limit_bytes=40 * 2 ** 20),
        cost_estimate=pl.CostEstimate(flops=5 * n_scores * (qk + v_dim), bytes_accessed=heads * seq * 16 * 256, transcendentals=n_scores),
        name="attn_fwd_bwd",
    )(rank, q, k, v, kp, do0, do1, cos_t, sin_t, *chain)


def merge_kernel(rank_ref, mine_ref, other_ref, out_ref):
    is_mine = pl.program_id(0) == rank_ref[0]

    @pl.when(is_mine)
    def _():
        out_ref[...] = mine_ref[...]

    @pl.when(jnp.logical_not(is_mine))
    def _():
        out_ref[...] = other_ref[...]


def merge_halves(rank, mine, other, axis, tile):
    lead, mid, width = mine.shape
    if axis == 0:
        block, steps = (tile, mid, width), lead // tile
        out_map = lambda half, i, r: (half * steps + i, 0, 0)
        out_shape = (2 * lead, mid, width)
    else:
        block, steps = (tile, mid, width), lead // tile
        out_map = lambda half, i, r: (i, half, 0)
        out_shape = (lead, 2 * mid, width)
    last = steps - 1
    mine_map = lambda half, i, r: (jnp.where(half == r[0], i, jnp.where(half == 0, 0, last)), 0, 0)
    other_map = lambda half, i, r: (jnp.where(half != r[0], i, jnp.where(half == 0, 0, last)), 0, 0)
    n_bytes = 4 * mine.size * 4
    return pl.pallas_call(
        merge_kernel,
        out_shape=jax.ShapeDtypeStruct(out_shape, mine.dtype),
        grid_spec=pltpu.PrefetchScalarGridSpec(
            num_scalar_prefetch=1, grid=(2, steps),
            in_specs=[pl.BlockSpec(block, mine_map), pl.BlockSpec(block, other_map)],
            out_specs=pl.BlockSpec(block, out_map)),
        compiler_params=pltpu.CompilerParams(dimension_semantics=("arbitrary", "arbitrary"), vmem_limit_bytes=48 * 2 ** 20),
        cost_estimate=pl.CostEstimate(flops=n_bytes * 100, bytes_accessed=n_bytes, transcendentals=0),
        name="merge_halves",
    )(rank, mine, other)


def head_wgrad_kernel(rank_ref, act_ref, in0_ref, in1_ref, full_ref, mine_ref):
    n_batch = act_ref.shape[2]
    total = None
    for slot, in_ref in ((0, in0_ref), (1, in1_ref)):
        for b in range(n_batch):
            act = act_ref[slot, :, b].reshape(-1, act_ref.shape[4])
            part = dot(act, in_ref[b], 1, 0)
            total = part if total is None else total + part
    total = total.reshape(mine_ref.shape)
    full_ref[...] = total
    mine_ref[...] = total


def head_wgrad(rank, act, in0, in1, tile_h, tile_d):
    _, heads, n_batch, width, seq = act.shape
    d_dim = in0.shape[-1]
    n_h, n_d = heads // tile_h, d_dim // tile_d
    in_spec = pl.BlockSpec((n_batch, seq, tile_d), lambda d, h, r: (0, 0, d))
    return pl.pallas_call(
        head_wgrad_kernel,
        out_shape=[jax.ShapeDtypeStruct((2 * heads, width, d_dim), F32), jax.ShapeDtypeStruct((heads, width, d_dim), F32)],
        grid_spec=pltpu.PrefetchScalarGridSpec(
            num_scalar_prefetch=1, grid=(n_d, n_h),
            in_specs=[pl.BlockSpec((2, tile_h, n_batch, width, seq), lambda d, h, r: (0, h, 0, 0, 0)), in_spec, in_spec],
            out_specs=[pl.BlockSpec((tile_h, width, tile_d), lambda d, h, r: (r[0] * n_h + h, 0, d)),
                       pl.BlockSpec((tile_h, width, tile_d), lambda d, h, r: (h, 0, d))]),
        compiler_params=pltpu.CompilerParams(dimension_semantics=("arbitrary", "arbitrary"), vmem_limit_bytes=56 * 2 ** 20),
        cost_estimate=pl.CostEstimate(flops=4 * heads * width * n_batch * seq * d_dim, bytes_accessed=8 * heads * width * d_dim, transcendentals=0),
        name="head_wgrad",
    )(rank, act, in0, in1)


def fill_kernel(rank_ref, other_ref, whole_ref, out_ref):
    out_ref[...] = other_ref[...]


def fill_other(rank, whole, other, tile_h):
    heads, width, d_dim = other.shape
    n_h = heads // tile_h
    return pl.pallas_call(
        fill_kernel,
        out_shape=jax.ShapeDtypeStruct(whole.shape, whole.dtype),
        grid_spec=pltpu.PrefetchScalarGridSpec(
            num_scalar_prefetch=1, grid=(n_h,),
            in_specs=[pl.BlockSpec((tile_h, width, d_dim), lambda h, r: (h, 0, 0)), pl.BlockSpec(memory_space=pl.ANY)],
            out_specs=pl.BlockSpec((tile_h, width, d_dim), lambda h, r: ((1 - r[0]) * n_h + h, 0, 0))),
        input_output_aliases={2: 0},
        compiler_params=pltpu.CompilerParams(dimension_semantics=("arbitrary",), vmem_limit_bytes=48 * 2 ** 20),
        cost_estimate=pl.CostEstimate(flops=100 * 8 * other.size, bytes_accessed=8 * other.size, transcendentals=0),
        name="fill_other",
    )(rank, other, whole)


def down_wgrad_kernel(x0_ref, x1_ref, q0_ref, q1_ref, c0_ref, c1_ref, dq_ref, dc_ref):
    x0 = x0_ref[...]
    x1 = x1_ref[...]
    dq_ref[...] = dot(x0, q0_ref[...], 0, 0) + dot(x1, q1_ref[...], 0, 0)
    dc_ref[...] = dot(c0_ref[...], x0, 0, 0) + dot(c1_ref[...], x1, 0, 0)


def down_wgrad(x0, x1, q0, q1, c0, c1):
    width, q_dim, c_dim = x0.shape[-1], q0.shape[-1], c0.shape[-1]
    operands = [value.reshape(-1, value.shape[-1]) for value in (x0, x1, q0, q1, c0, c1)]
    tokens = operands[0].shape[0]
    tile = min(width, 256)
    x_spec = pl.BlockSpec((tokens, tile), lambda i: (0, i))
    q_spec = pl.BlockSpec((tokens, q_dim), lambda i: (0, 0))
    c_spec = pl.BlockSpec((tokens, c_dim), lambda i: (0, 0))
    grad_q, grad_c = pl.pallas_call(
        down_wgrad_kernel,
        out_shape=[jax.ShapeDtypeStruct((width, q_dim), F32), jax.ShapeDtypeStruct((c_dim, width), F32)],
        grid=(width // tile,),
        in_specs=[x_spec, x_spec, q_spec, q_spec, c_spec, c_spec],
        out_specs=[pl.BlockSpec((tile, q_dim), lambda i: (i, 0)), pl.BlockSpec((c_dim, tile), lambda i: (0, i))],
        compiler_params=pltpu.CompilerParams(dimension_semantics=("arbitrary",), vmem_limit_bytes=56 * 2 ** 20),
        cost_estimate=pl.CostEstimate(flops=4 * tokens * width * (q_dim + c_dim), bytes_accessed=4 * tokens * width + 4 * width * (q_dim + c_dim), transcendentals=0),
        name="down_wgrad",
    )(*operands)
    return grad_q, grad_c.T


def solution(mesh):
    cp_size = mesh.shape['cp']
    tp_size = mesh.shape['tp']
    swap_pairs = [(0, 1), (1, 0)]

    def swap(value):
        return lax.ppermute(value, 'cp', swap_pairs)

    def with_other(value):
        return jnp.stack([value, swap(value)])

    def block(hidden, grad_out, w_dq, g_q, w_dkv, g_kv, w_uq, w_uk, w_uv, w_o):
        cp_rank = lax.axis_index('cp')
        tp_rank = lax.axis_index('tp')
        rank = cp_rank.astype(jnp.int32)[None]
        n_batch, seq_local, _ = hidden.shape
        q_lora = w_dq.shape[1]
        kv_lora = g_kv.shape[0]
        nope_dim = w_uk.shape[2]
        v_dim = w_uv.shape[2]
        qk_dim = w_uq.shape[2]
        rope_dim = qk_dim - nope_dim
        heads_core = w_uq.shape[1] // cp_size
        tok_tp = seq_local // tp_size

        positions = layout_positions(seq_local, cp_size, cp_rank)
        cos_tab, sin_tab = rope_tables(positions, rope_dim)
        cos_nat, sin_nat = rope_tables(jnp.arange(cp_size * seq_local, dtype=jnp.int32), rope_dim)
        cos_t, sin_t = cos_nat.T, sin_nat.T

        head0 = cp_rank * heads_core
        uq_mine = lax.dynamic_slice_in_dim(jnp.transpose(w_uq, (1, 2, 0)), head0, heads_core, 0)
        uk_mine = lax.dynamic_slice_in_dim(w_uk, head0, heads_core, 1).reshape(kv_lora, heads_core * nope_dim)
        uv_mine = lax.dynamic_slice_in_dim(w_uv, head0, heads_core, 1).reshape(kv_lora, heads_core * v_dim)
        wo_mine = lax.dynamic_slice_in_dim(w_o, head0, heads_core, 0)

        cq_raw = jnp.einsum('btd,dq->btq', hidden, w_dq, preferred_element_type=F32).astype(BF16)
        kv_raw = jnp.einsum('btd,dc->btc', hidden, w_dkv, preferred_element_type=F32).astype(BF16)
        gq_f32 = g_q.astype(F32)
        gkv_f32 = g_kv.astype(F32)
        c_q = norm_f32(cq_raw.astype(F32), gq_f32).astype(BF16)
        c_kv = norm_f32(kv_raw[..., :kv_lora].astype(F32), gkv_f32).astype(BF16)
        k_pe = apply_rope(kv_raw[..., kv_lora:].astype(F32), cos_tab, sin_tab).astype(BF16)

        c_q2 = with_other(c_q)
        c_kv2 = with_other(c_kv)
        k_pe2 = with_other(k_pe)
        dy_other = swap(grad_out)

        def head_grads(dy):
            return jnp.einsum('hvd,btd->hbvt', wo_mine, dy, preferred_element_type=F32).astype(BF16)

        do0 = head_grads(grad_out)
        do1 = head_grads(dy_other)
        q_all = jnp.einsum('heq,sbtq->hsbet', uq_mine, c_q2, preferred_element_type=F32).astype(BF16)
        k_nope = jnp.einsum('sbtc,cn->sbtn', c_kv2, uk_mine, preferred_element_type=F32).astype(BF16)
        v_heads = jnp.einsum('sbtc,cv->sbtv', c_kv2, uv_mine, preferred_element_type=F32).astype(BF16)

        x_late, q_all = lax.optimization_barrier((hidden, q_all))
        x_other = swap(x_late)

        chain = ()
        dkp_parts = []
        y_parts = []
        for b in range(n_batch):
            res = attention(b, rank, q_all, k_nope, v_heads, k_pe2, do0, do1, cos_t, sin_t, chain)
            o_now, chain, dkp = res[0], tuple(res[1:5]), res[5]
            dkp_parts.append(dkp)
            o_recv = swap(o_now[1])
            o_full = jnp.concatenate([jnp.where(cp_rank == 0, o_now[0], o_recv), jnp.where(cp_rank == 0, o_recv, o_now[0])], axis=0)
            y_b = jnp.einsum('hvt,hvd->td', o_full, w_o, preferred_element_type=F32)
            chain, y_b = lax.optimization_barrier((chain, y_b))
            y_parts.append(lax.psum_scatter(y_b, 'tp', scatter_dimension=0, tiled=True).astype(BF16))
        o_all, dq_all, dk_all, dv_all = chain

        def latent_grads(slot):
            dcq = jnp.einsum('hbet,heq->btq', dq_all[slot], uq_mine, preferred_element_type=F32)
            dckv = jnp.einsum('btn,cn->btc', dk_all[slot], uk_mine, preferred_element_type=F32) + jnp.einsum('btv,cv->btc', dv_all[slot], uv_mine, preferred_element_type=F32)
            return dcq, dckv

        dcq_away, dckv_away = latent_grads(1)
        dcq_home, dckv_home = latent_grads(0)
        dkp2 = jnp.stack(dkp_parts, axis=1)
        latent_part = jnp.concatenate([
            dcq_home + swap(dcq_away),
            dckv_home + swap(dckv_away),
            dkp2[0] + swap(dkp2[1])], axis=-1)
        latent_part, y_parts, o_all, dq_late = lax.optimization_barrier((latent_part, y_parts, o_all, dq_all))
        latent_grad = lax.psum_scatter(latent_part, 'tp', scatter_dimension=1, tiled=True)

        wo_whole, wo_half = head_wgrad(rank, o_all, grad_out, dy_other, min(4, heads_core), min(1024, hidden.shape[2]))
        wo_swapped = swap(wo_half)
        uq_whole, uq_half = head_wgrad(rank, dq_late, c_q2[0], c_q2[1], min(4, heads_core), min(768, q_lora))
        uq_swapped = swap(uq_half)
        grad_w_uk = jnp.einsum('sbtc,sbtn->cn', c_kv2, dk_all, preferred_element_type=F32).reshape(kv_lora, heads_core, nope_dim)
        grad_w_uv = jnp.einsum('sbtc,sbtv->cv', c_kv2, dv_all, preferred_element_type=F32).reshape(kv_lora, heads_core, v_dim)
        latent_grad, grad_w_uk, grad_w_uv, uq_whole = lax.optimization_barrier((latent_grad, grad_w_uk, grad_w_uv, uq_whole))

        def my_tokens(value, axis):
            return lax.dynamic_slice_in_dim(value, tp_rank * tok_tp, tok_tp, axis)

        cq_mine = my_tokens(cq_raw, 1).astype(F32)
        ckv_mine = my_tokens(kv_raw, 1)[..., :kv_lora].astype(F32)
        grad_cq_raw, grad_g_q = jax.vjp(norm_f32, cq_mine, gq_f32)[1](latent_grad[..., :q_lora])
        grad_ckv_raw, grad_g_kv = jax.vjp(norm_f32, ckv_mine, gkv_f32)[1](latent_grad[..., q_lora:q_lora + kv_lora])
        grad_kpe_raw = unrope(latent_grad[..., q_lora + kv_lora:], my_tokens(cos_tab, 0), my_tokens(sin_tab, 0))
        draw = jnp.concatenate([grad_cq_raw, grad_ckv_raw, grad_kpe_raw], axis=-1).astype(BF16)
        draw = lax.all_gather(draw, 'tp', axis=1, tiled=True)
        grad_g = jnp.concatenate([grad_g_q, grad_g_kv])
        for bit in (1, 2):
            grad_g = grad_g + lax.ppermute(grad_g, 'tp', [(src, src ^ bit) for src in range(tp_size)])
        grad_g = grad_g + swap(grad_g)
        grad_g_q, grad_g_kv = grad_g[:q_lora], grad_g[q_lora:]

        y_stack, draw = lax.optimization_barrier((jnp.stack(y_parts), draw))
        attn_out = lax.all_gather(y_stack, 'tp', axis=1, tiled=True)

        grad_w_o = fill_other(rank, wo_whole, wo_swapped, 1)
        grad_w_uq = jnp.transpose(fill_other(rank, uq_whole, uq_swapped, 2), (2, 0, 1))
        grad_w_uk = merge_halves(rank, grad_w_uk, swap(grad_w_uk), 1, min(kv_lora, 256))
        grad_w_uv = merge_halves(rank, grad_w_uv, swap(grad_w_uv), 1, min(kv_lora, 256))

        dcq_raw, dkv_raw = lax.optimization_barrier((draw[..., :q_lora], draw[..., q_lora:]))
        dcq_other, dkv_other = swap(dcq_raw), swap(dkv_raw)
        grad_hidden = (jnp.einsum('btq,dq->btd', dcq_raw, w_dq, preferred_element_type=F32) + jnp.einsum('btc,dc->btd', dkv_raw, w_dkv, preferred_element_type=F32)).astype(BF16)
        grad_w_dq, grad_w_dkv = down_wgrad(hidden, x_other, dcq_raw, dcq_other, dkv_raw, dkv_other)
        return (attn_out, grad_hidden, grad_w_dq, grad_g_q, grad_w_dkv, grad_g_kv, grad_w_uq, grad_w_uk, grad_w_uv, grad_w_o)

    seq_spec = P(None, 'cp', None)
    full_spec = P()
    head_spec = P(None, 'tp', None)
    out_head_spec = P('tp', None, None)
    all_specs = (seq_spec, seq_spec, full_spec, full_spec, full_spec, full_spec, head_spec, head_spec, head_spec, out_head_spec)
    return jax.shard_map(block, mesh=mesh, in_specs=all_specs, out_specs=all_specs, check_vma=False)
```

```python
import functools

import jax
import jax.numpy as jnp
from jax import lax
from jax.experimental import pallas as pl
from jax.experimental.pallas import tpu as pltpu
from jax.sharding import PartitionSpec as P


EPS = 1e-6
THETA = 10000.0
NEG_BIG = -1e30
LOG2E = 1.4426950408889634
BLOCK_SLOT = (0, 1, 1, 0)
BLOCK_HALF = (0, 0, 1, 1)
F32 = jnp.float32
BF16 = jnp.bfloat16


def layout_positions(seq_local, cp_size, cp_rank):
    half_len = seq_local // 2
    local_idx = jnp.arange(seq_local, dtype=jnp.int32)
    block_id = jnp.where(local_idx < half_len, cp_rank, 2 * cp_size - 1 - cp_rank)
    return block_id * half_len + local_idx % half_len


def rope_tables(positions, rope_dim):
    inv_freq = 1.0 / (THETA ** (jnp.arange(rope_dim // 2, dtype=F32) * 2.0 / rope_dim))
    angles = positions.astype(F32)[:, None] * inv_freq[None, :]
    return jnp.cos(angles), jnp.sin(angles)


def apply_rope(values, cos_tab, sin_tab):
    half_dim = values.shape[-1] // 2
    lead_half = values[..., :half_dim]
    tail_half = values[..., half_dim:]
    return jnp.concatenate([lead_half * cos_tab - tail_half * sin_tab, tail_half * cos_tab + lead_half * sin_tab], axis=-1)


def unrope(grad_vals, cos_tab, sin_tab):
    half_dim = grad_vals.shape[-1] // 2
    lead_half = grad_vals[..., :half_dim]
    tail_half = grad_vals[..., half_dim:]
    return jnp.concatenate([lead_half * cos_tab + tail_half * sin_tab, tail_half * cos_tab - lead_half * sin_tab], axis=-1)


def norm_f32(raw_vals, gain_vec):
    inv_rms = lax.rsqrt(jnp.mean(raw_vals * raw_vals, axis=-1, keepdims=True) + EPS)
    return raw_vals * inv_rms * gain_vec


def dot(lhs, rhs, lhs_dim, rhs_dim):
    return lax.dot_general(lhs, rhs, (((lhs_dim,), (rhs_dim,)), ((), ())), preferred_element_type=F32)


def attn_kernel(scale, n_alias, rank_ref, q_ref, k_ref, v_ref, kp_ref, do0_ref, do1_ref, cos_ref, sin_ref, *rest):
    o_now_ref, o_ref, dq_ref, dk_ref, dv_ref, dkp_ref, kcat, k_t, v_t, qcat, dk_acc, dv_acc, score, prob_b, grad_s = rest[n_alias:]
    rank = rank_ref[0]
    blk = q_ref.shape[4] // 2
    nope = k_ref.shape[3]
    qk = q_ref.shape[3]
    half = (qk - nope) // 2
    mid = nope + half
    place = [(jnp.bitwise_xor(rank, BLOCK_SLOT[p]), slice(BLOCK_HALF[p] * blk, BLOCK_HALF[p] * blk + blk)) for p in range(4)]

    def span(p):
        return slice(p * blk, p * blk + blk)

    @pl.when(pl.program_id(0) == 0)
    def _():
        dkp_ref[...] = jnp.zeros_like(dkp_ref)
        for p in range(4):
            slot, rows = place[p]
            k_rope = kp_ref[slot, 0, rows, :]
            kcat[span(p), nope:] = k_rope
            k_t[nope:, span(p)] = k_rope.T

    for p in range(4):
        slot, rows = place[p]
        k_blk = k_ref[slot, 0, rows, :]
        kcat[span(p), :nope] = k_blk
        k_t[:nope, span(p)] = k_blk.T
        v_t[:, span(p)] = v_ref[slot, 0, rows, :].T

    untouched = [True] * 4
    pending = [4 - j for j in range(4)]

    def flush(j):
        slot, rows = place[j]
        dk_ref[slot, 0, rows, :] = (dk_acc[span(j), :nope] * scale).astype(BF16)
        dv_ref[slot, 0, rows, :] = dv_acc[span(j), :].astype(BF16)
        dkp_ref[slot, rows, :] += dk_acc[span(j), nope:] * scale

    def steps(p, buf):
        slot, rows = place[p]
        n_blk = p + 1
        yield False, 0
        cos_p = cos_ref[:, span(p)]
        sin_p = sin_ref[:, span(p)]
        lead = q_ref[0, slot, 0, nope:mid, rows].astype(F32)
        tail = q_ref[0, slot, 0, mid:, rows].astype(F32)
        qcat[p, :nope, :] = q_ref[0, slot, 0, :nope, rows]
        qcat[p, nope:mid, :] = (lead * cos_p - tail * sin_p).astype(BF16)
        qcat[p, mid:, :] = (tail * cos_p + lead * sin_p).astype(BF16)
        col_max = None
        for j in range(n_blk):
            yield True, 2
            st = dot(kcat[span(j), :], qcat[p], 1, 0)
            if j == p:
                key_id = lax.broadcasted_iota(jnp.int32, (blk, blk), 0)
                qry_id = lax.broadcasted_iota(jnp.int32, (blk, blk), 1)
                st = jnp.where(key_id <= qry_id, st, NEG_BIG)
            score[buf, span(j), :] = st
            part = jnp.max(st, axis=0, keepdims=True)
            col_max = part if col_max is None else jnp.maximum(col_max, part)
        col_sum = None
        for j in range(n_blk):
            yield False, 3
            prob = jnp.exp2((score[buf, span(j), :] - col_max) * (scale * LOG2E))
            score[buf, span(j), :] = prob
            part = jnp.sum(prob, axis=0, keepdims=True)
            col_sum = part if col_sum is None else col_sum + part
        inv_sum = 1.0 / col_sum
        for j in range(n_blk):
            yield False, 2
            prob_b[buf, span(j), :] = (score[buf, span(j), :] * inv_sum).astype(BF16)
        n_keys = n_blk * blk
        yield True, n_blk
        out = dot(v_t[:, :n_keys], prob_b[buf, :n_keys, :], 1, 0)
        out_b = out.astype(BF16)
        o_ref[slot, 0, 0, :, rows] = out_b
        o_now_ref[slot, 0, :, rows] = out_b
        do_blk = jnp.where(slot == 0, do0_ref[0, 0, :, rows], do1_ref[0, 0, :, rows])
        row_dot = jnp.sum(out * do_blk.astype(F32), axis=0, keepdims=True)
        for j in range(n_blk):
            yield True, 2
            v_slot, v_rows = place[j]
            dprob = dot(v_ref[v_slot, 0, v_rows, :], do_blk, 1, 0)
            grad_s[buf, span(j), :] = (score[buf, span(j), :] * ((dprob - row_dot) * inv_sum)).astype(BF16)
        for j in range(n_blk):
            yield True, 4
            dk_part = dot(grad_s[buf, span(j), :], qcat[p], 1, 1)
            dv_part = dot(prob_b[buf, span(j), :], do_blk, 1, 1)
            if untouched[j]:
                dk_acc[span(j), :] = dk_part
                dv_acc[span(j), :] = dv_part
                untouched[j] = False
            else:
                dk_acc[span(j), :] += dk_part
                dv_acc[span(j), :] += dv_part
            pending[j] -= 1
            if pending[j] == 0:
                flush(j)
        yield True, n_blk
        dq = dot(k_t[:, :n_keys], grad_s[buf, :n_keys, :], 1, 0) * scale
        lead = dq[nope:mid, :]
        tail = dq[mid:, :]
        dq_ref[slot, 0, 0, :nope, rows] = dq[:nope, :].astype(BF16)
        dq_ref[slot, 0, 0, nope:mid, rows] = (lead * cos_p + tail * sin_p).astype(BF16)
        dq_ref[slot, 0, 0, mid:, rows] = (tail * cos_p - lead * sin_p).astype(BF16)

    def stream(blocks, buf):
        for p in blocks:
            yield from steps(p, buf)

    streams = [stream((3, 0), 0), stream((2, 1), 1)]
    heads_of = [next(st) for st in streams]
    busy = {True: 0, False: 0}
    while any(nxt is not None for nxt in heads_of):
        ready = [i for i in range(2) if heads_of[i] is not None]
        pick = min(ready, key=lambda i: (busy[heads_of[i][0]], i))
        is_mxu, cost = heads_of[pick]
        busy[is_mxu] += cost
        heads_of[pick] = next(streams[pick], None)


def attention(batch, rank, q, k, v, kp, do0, do1, cos_t, sin_t, chain):
    heads, _, n_batch, qk, seq = q.shape
    v_dim = do0.shape[2]
    rope = kp.shape[3]
    nope = qk - rope

    def whole(*shape):
        return pl.BlockSpec(shape, lambda h, r: (0,) * len(shape))

    q_spec = pl.BlockSpec((1, 2, 1, qk, seq), lambda h, r: (h, 0, batch, 0, 0))
    k_spec = pl.BlockSpec((2, 1, seq, nope), lambda h, r: (0, batch, 0, h))
    v_spec = pl.BlockSpec((2, 1, seq, v_dim), lambda h, r: (0, batch, 0, h))
    do_spec = pl.BlockSpec((1, 1, v_dim, seq), lambda h, r: (h, batch, 0, 0))
    o_spec = pl.BlockSpec((2, 1, 1, v_dim, seq), lambda h, r: (0, h, batch, 0, 0))
    dq_spec = pl.BlockSpec((2, 1, 1, qk, seq), lambda h, r: (0, h, batch, 0, 0))
    shared = [jax.ShapeDtypeStruct((2, heads, n_batch, v_dim, seq), BF16), jax.ShapeDtypeStruct((2, heads, n_batch, qk, seq), BF16),
              jax.ShapeDtypeStruct(k.shape, BF16), jax.ShapeDtypeStruct(v.shape, BF16)]
    n_alias = len(chain)
    n_scores = heads * (4 * seq * seq) * 5 // 8
    return pl.pallas_call(
        functools.partial(attn_kernel, qk ** -0.5, n_alias),
        out_shape=[jax.ShapeDtypeStruct((2, heads, v_dim, seq), BF16)] + shared + [jax.ShapeDtypeStruct((2, seq, rope), F32)],
        grid_spec=pltpu.PrefetchScalarGridSpec(
            num_scalar_prefetch=1,
            grid=(heads,),
            in_specs=[q_spec, k_spec, v_spec, pl.BlockSpec((2, 1, seq, rope), lambda h, r: (0, batch, 0, 0)),
                      do_spec, do_spec, whole(rope // 2, 2 * seq), whole(rope // 2, 2 * seq)]
            + [pl.BlockSpec(memory_space=pl.ANY)] * n_alias,
            out_specs=[pl.BlockSpec((2, 1, v_dim, seq), lambda h, r: (0, h, 0, 0)),
                       o_spec, dq_spec, k_spec, v_spec, whole(2, seq, rope)],
            scratch_shapes=[pltpu.VMEM((2 * seq, qk), BF16), pltpu.VMEM((qk, 2 * seq), BF16), pltpu.VMEM((v_dim, 2 * seq), BF16),
                            pltpu.VMEM((4, qk, seq // 2), BF16),
                            pltpu.VMEM((2 * seq, qk), F32), pltpu.VMEM((2 * seq, v_dim), F32),
                            pltpu.VMEM((2, 2 * seq, seq // 2), F32), pltpu.VMEM((2, 2 * seq, seq // 2), BF16),
                            pltpu.VMEM((2, 2 * seq, seq // 2), BF16)],
        ),
        input_output_aliases={9 + i: 1 + i for i in range(n_alias)},
        compiler_params=pltpu.CompilerParams(dimension_semantics=("arbitrary",), vmem_limit_bytes=40 * 2 ** 20),
        cost_estimate=pl.CostEstimate(flops=5 * n_scores * (qk + v_dim), bytes_accessed=heads * seq * 16 * 256, transcendentals=n_scores),
        name="attn_fwd_bwd",
    )(rank, q, k, v, kp, do0, do1, cos_t, sin_t, *chain)


def merge_kernel(rank_ref, mine_ref, other_ref, out_ref):
    is_mine = pl.program_id(0) == rank_ref[0]

    @pl.when(is_mine)
    def _():
        out_ref[...] = mine_ref[...]

    @pl.when(jnp.logical_not(is_mine))
    def _():
        out_ref[...] = other_ref[...]


def merge_halves(rank, mine, other, axis, tile):
    lead, mid, width = mine.shape
    if axis == 0:
        block, steps = (tile, mid, width), lead // tile
        out_map = lambda half, i, r: (half * steps + i, 0, 0)
        out_shape = (2 * lead, mid, width)
    else:
        block, steps = (tile, mid, width), lead // tile
        out_map = lambda half, i, r: (i, half, 0)
        out_shape = (lead, 2 * mid, width)
    last = steps - 1
    mine_map = lambda half, i, r: (jnp.where(half == r[0], i, jnp.where(half == 0, 0, last)), 0, 0)
    other_map = lambda half, i, r: (jnp.where(half != r[0], i, jnp.where(half == 0, 0, last)), 0, 0)
    n_bytes = 4 * mine.size * 4
    return pl.pallas_call(
        merge_kernel,
        out_shape=jax.ShapeDtypeStruct(out_shape, mine.dtype),
        grid_spec=pltpu.PrefetchScalarGridSpec(
            num_scalar_prefetch=1, grid=(2, steps),
            in_specs=[pl.BlockSpec(block, mine_map), pl.BlockSpec(block, other_map)],
            out_specs=pl.BlockSpec(block, out_map)),
        compiler_params=pltpu.CompilerParams(dimension_semantics=("arbitrary", "arbitrary"), vmem_limit_bytes=48 * 2 ** 20),
        cost_estimate=pl.CostEstimate(flops=n_bytes * 100, bytes_accessed=n_bytes, transcendentals=0),
        name="merge_halves",
    )(rank, mine, other)


def head_wgrad_kernel(rank_ref, act_ref, in0_ref, in1_ref, full_ref, mine_ref):
    n_batch = act_ref.shape[2]
    tile_h = mine_ref.shape[0]
    head0 = pl.program_id(1) * tile_h
    total = None
    for slot, in_ref in ((0, in0_ref), (1, in1_ref)):
        for b in range(n_batch):
            act = act_ref[slot, pl.ds(head0, tile_h), b].reshape(-1, act_ref.shape[4])
            part = dot(act, in_ref[b], 1, 0)
            total = part if total is None else total + part
    total = total.reshape(mine_ref.shape)
    full_ref[...] = total
    mine_ref[...] = total


def head_wgrad(rank, act, in0, in1, tile_h, tile_d):
    _, heads, n_batch, width, seq = act.shape
    d_dim = in0.shape[-1]
    n_h, n_d = heads // tile_h, d_dim // tile_d
    in_spec = pl.BlockSpec((n_batch, seq, tile_d), lambda d, h, r: (0, 0, d))
    return pl.pallas_call(
        head_wgrad_kernel,
        out_shape=[jax.ShapeDtypeStruct((2 * heads, width, d_dim), F32), jax.ShapeDtypeStruct((heads, width, d_dim), F32)],
        grid_spec=pltpu.PrefetchScalarGridSpec(
            num_scalar_prefetch=1, grid=(n_d, n_h),
            in_specs=[pl.BlockSpec(act.shape, lambda d, h, r: (0, 0, 0, 0, 0), pipeline_mode=pl.Buffered(1)), in_spec, in_spec],
            out_specs=[pl.BlockSpec((tile_h, width, tile_d), lambda d, h, r: (r[0] * n_h + h, 0, d)),
                       pl.BlockSpec((tile_h, width, tile_d), lambda d, h, r: (h, 0, d))]),
        compiler_params=pltpu.CompilerParams(dimension_semantics=("arbitrary", "arbitrary"), vmem_limit_bytes=56 * 2 ** 20),
        cost_estimate=pl.CostEstimate(flops=4 * heads * width * n_batch * seq * d_dim, bytes_accessed=8 * heads * width * d_dim, transcendentals=0),
        name="head_wgrad",
    )(rank, act, in0, in1)


def fill_kernel(rank_ref, other_ref, whole_ref, out_ref):
    out_ref[...] = other_ref[...]


def fill_other(rank, whole, other, tile_h):
    heads, width, d_dim = other.shape
    n_h = heads // tile_h
    return pl.pallas_call(
        fill_kernel,
        out_shape=jax.ShapeDtypeStruct(whole.shape, whole.dtype),
        grid_spec=pltpu.PrefetchScalarGridSpec(
            num_scalar_prefetch=1, grid=(n_h,),
            in_specs=[pl.BlockSpec((tile_h, width, d_dim), lambda h, r: (h, 0, 0)), pl.BlockSpec(memory_space=pl.ANY)],
            out_specs=pl.BlockSpec((tile_h, width, d_dim), lambda h, r: ((1 - r[0]) * n_h + h, 0, 0))),
        input_output_aliases={2: 0},
        compiler_params=pltpu.CompilerParams(dimension_semantics=("arbitrary",), vmem_limit_bytes=48 * 2 ** 20),
        cost_estimate=pl.CostEstimate(flops=100 * 8 * other.size, bytes_accessed=8 * other.size, transcendentals=0),
        name="fill_other",
    )(rank, other, whole)


def down_wgrad_kernel(x0_ref, x1_ref, q0_ref, q1_ref, c0_ref, c1_ref, dq_ref, dc_ref):
    x0 = x0_ref[...]
    x1 = x1_ref[...]
    dq_ref[...] = dot(x0, q0_ref[...], 0, 0) + dot(x1, q1_ref[...], 0, 0)
    dc_ref[...] = dot(c0_ref[...], x0, 0, 0) + dot(c1_ref[...], x1, 0, 0)


def down_wgrad(x0, x1, q0, q1, c0, c1):
    width, q_dim, c_dim = x0.shape[-1], q0.shape[-1], c0.shape[-1]
    operands = [value.reshape(-1, value.shape[-1]) for value in (x0, x1, q0, q1, c0, c1)]
    tokens = operands[0].shape[0]
    tile = min(width, 256)
    x_spec = pl.BlockSpec((tokens, tile), lambda i: (0, i))
    q_spec = pl.BlockSpec((tokens, q_dim), lambda i: (0, 0))
    c_spec = pl.BlockSpec((tokens, c_dim), lambda i: (0, 0))
    grad_q, grad_c = pl.pallas_call(
        down_wgrad_kernel,
        out_shape=[jax.ShapeDtypeStruct((width, q_dim), F32), jax.ShapeDtypeStruct((c_dim, width), F32)],
        grid=(width // tile,),
        in_specs=[x_spec, x_spec, q_spec, q_spec, c_spec, c_spec],
        out_specs=[pl.BlockSpec((tile, q_dim), lambda i: (i, 0)), pl.BlockSpec((c_dim, tile), lambda i: (0, i))],
        compiler_params=pltpu.CompilerParams(dimension_semantics=("arbitrary",), vmem_limit_bytes=56 * 2 ** 20),
        cost_estimate=pl.CostEstimate(flops=4 * tokens * width * (q_dim + c_dim), bytes_accessed=4 * tokens * width + 4 * width * (q_dim + c_dim), transcendentals=0),
        name="down_wgrad",
    )(*operands)
    return grad_q, grad_c.T


def solution(mesh):
    cp_size = mesh.shape['cp']
    tp_size = mesh.shape['tp']
    swap_pairs = [(0, 1), (1, 0)]

    def swap(value):
        return lax.ppermute(value, 'cp', swap_pairs)

    def with_other(value):
        return jnp.stack([value, swap(value)])

    def block(hidden, grad_out, w_dq, g_q, w_dkv, g_kv, w_uq, w_uk, w_uv, w_o):
        cp_rank = lax.axis_index('cp')
        tp_rank = lax.axis_index('tp')
        rank = cp_rank.astype(jnp.int32)[None]
        n_batch, seq_local, _ = hidden.shape
        q_lora = w_dq.shape[1]
        kv_lora = g_kv.shape[0]
        nope_dim = w_uk.shape[2]
        v_dim = w_uv.shape[2]
        qk_dim = w_uq.shape[2]
        rope_dim = qk_dim - nope_dim
        heads_core = w_uq.shape[1] // cp_size
        tok_tp = seq_local // tp_size

        positions = layout_positions(seq_local, cp_size, cp_rank)
        cos_tab, sin_tab = rope_tables(positions, rope_dim)
        cos_nat, sin_nat = rope_tables(jnp.arange(cp_size * seq_local, dtype=jnp.int32), rope_dim)
        cos_t, sin_t = cos_nat.T, sin_nat.T

        head0 = cp_rank * heads_core
        uq_mine = lax.dynamic_slice_in_dim(jnp.transpose(w_uq, (1, 2, 0)), head0, heads_core, 0)
        uk_mine = lax.dynamic_slice_in_dim(w_uk, head0, heads_core, 1).reshape(kv_lora, heads_core * nope_dim)
        uv_mine = lax.dynamic_slice_in_dim(w_uv, head0, heads_core, 1).reshape(kv_lora, heads_core * v_dim)
        wo_mine = lax.dynamic_slice_in_dim(w_o, head0, heads_core, 0)

        cq_raw = jnp.einsum('btd,dq->btq', hidden, w_dq, preferred_element_type=F32).astype(BF16)
        kv_raw = jnp.einsum('btd,dc->btc', hidden, w_dkv, preferred_element_type=F32).astype(BF16)
        gq_f32 = g_q.astype(F32)
        gkv_f32 = g_kv.astype(F32)
        c_q = norm_f32(cq_raw.astype(F32), gq_f32).astype(BF16)
        c_kv = norm_f32(kv_raw[..., :kv_lora].astype(F32), gkv_f32).astype(BF16)
        k_pe = apply_rope(kv_raw[..., kv_lora:].astype(F32), cos_tab, sin_tab).astype(BF16)

        c_q2 = with_other(c_q)
        c_kv2 = with_other(c_kv)
        k_pe2 = with_other(k_pe)
        dy_other = swap(grad_out)

        def head_grads(dy):
            return jnp.einsum('hvd,btd->hbvt', wo_mine, dy, preferred_element_type=F32).astype(BF16)

        do0 = head_grads(grad_out)
        do1 = head_grads(dy_other)
        q_all = jnp.einsum('heq,sbtq->hsbet', uq_mine, c_q2, preferred_element_type=F32).astype(BF16)
        k_nope = jnp.einsum('sbtc,cn->sbtn', c_kv2, uk_mine, preferred_element_type=F32).astype(BF16)
        v_heads = jnp.einsum('sbtc,cv->sbtv', c_kv2, uv_mine, preferred_element_type=F32).astype(BF16)

        x_late, q_all = lax.optimization_barrier((hidden, q_all))
        x_other = swap(x_late)

        chain = ()
        dkp_parts = []
        y_parts = []
        for b in range(n_batch):
            res = attention(b, rank, q_all, k_nope, v_heads, k_pe2, do0, do1, cos_t, sin_t, chain)
            o_now, chain, dkp = res[0], tuple(res[1:5]), res[5]
            dkp_parts.append(dkp)
            o_recv = swap(o_now[1])
            o_full = jnp.concatenate([jnp.where(cp_rank == 0, o_now[0], o_recv), jnp.where(cp_rank == 0, o_recv, o_now[0])], axis=0)
            y_b = jnp.einsum('hvt,hvd->td', o_full, w_o, preferred_element_type=F32)
            chain, y_b = lax.optimization_barrier((chain, y_b))
            y_b = lax.psum_scatter(y_b, 'tp', scatter_dimension=0, tiled=True)
            y_parts.append(y_b.astype(BF16))
        o_all, dq_all, dk_all, dv_all = chain

        def latent_grads(slot):
            dcq = jnp.einsum('hbet,heq->btq', dq_all[slot], uq_mine, preferred_element_type=F32)
            dckv = jnp.einsum('btn,cn->btc', dk_all[slot], uk_mine, preferred_element_type=F32) + jnp.einsum('btv,cv->btc', dv_all[slot], uv_mine, preferred_element_type=F32)
            return dcq, dckv

        dcq_away, dckv_away = latent_grads(1)
        dcq_home, dckv_home = latent_grads(0)
        dkp2 = jnp.stack(dkp_parts, axis=1)
        latent_part = jnp.concatenate([
            dcq_home + swap(dcq_away),
            dckv_home + swap(dckv_away),
            dkp2[0] + swap(dkp2[1])], axis=-1)
        latent_part, o_all, dq_late = lax.optimization_barrier((latent_part, o_all, dq_all))
        latent_grad = lax.psum_scatter(latent_part, 'tp', scatter_dimension=1, tiled=True)

        wo_whole, wo_half = head_wgrad(rank, o_all, grad_out, dy_other, min(4, heads_core), min(1024, hidden.shape[2]))
        wo_swapped = swap(wo_half)
        uq_whole, uq_half = head_wgrad(rank, dq_late, c_q2[0], c_q2[1], min(4, heads_core), min(768, q_lora))
        uq_swapped = swap(uq_half)
        grad_w_uk = jnp.einsum('sbtc,sbtn->cn', c_kv2, dk_all, preferred_element_type=F32).reshape(kv_lora, heads_core, nope_dim)
        grad_w_uv = jnp.einsum('sbtc,sbtv->cv', c_kv2, dv_all, preferred_element_type=F32).reshape(kv_lora, heads_core, v_dim)
        latent_grad, grad_w_uk, grad_w_uv, uq_whole = lax.optimization_barrier((latent_grad, grad_w_uk, grad_w_uv, uq_whole))

        def my_tokens(value, axis):
            return lax.dynamic_slice_in_dim(value, tp_rank * tok_tp, tok_tp, axis)

        cq_mine = my_tokens(cq_raw, 1).astype(F32)
        ckv_mine = my_tokens(kv_raw, 1)[..., :kv_lora].astype(F32)
        grad_cq_raw, grad_g_q = jax.vjp(norm_f32, cq_mine, gq_f32)[1](latent_grad[..., :q_lora])
        grad_ckv_raw, grad_g_kv = jax.vjp(norm_f32, ckv_mine, gkv_f32)[1](latent_grad[..., q_lora:q_lora + kv_lora])
        grad_kpe_raw = unrope(latent_grad[..., q_lora + kv_lora:], my_tokens(cos_tab, 0), my_tokens(sin_tab, 0))
        draw = jnp.concatenate([grad_cq_raw, grad_ckv_raw, grad_kpe_raw], axis=-1).astype(BF16)
        draw = lax.all_gather(draw, 'tp', axis=1, tiled=True)
        grad_g = jnp.concatenate([grad_g_q, grad_g_kv])
        for bit in (1, 2):
            grad_g = grad_g + lax.ppermute(grad_g, 'tp', [(src, src ^ bit) for src in range(tp_size)])
        grad_g = grad_g + swap(grad_g)
        grad_g_q, grad_g_kv = grad_g[:q_lora], grad_g[q_lora:]

        y_stack, draw = lax.optimization_barrier((jnp.stack(y_parts), draw))
        attn_out = lax.all_gather(y_stack, 'tp', axis=1, tiled=True)

        grad_w_o = fill_other(rank, wo_whole, wo_swapped, 1)
        grad_w_uq = fill_other(rank, uq_whole, uq_swapped, 2)
        grad_w_uq = jnp.transpose(grad_w_uq, (2, 0, 1))
        uk_swapped, uv_swapped = swap(grad_w_uk), swap(grad_w_uv)
        grad_w_uk = merge_halves(rank, grad_w_uk, uk_swapped, 1, min(kv_lora, 256))
        grad_w_uv = merge_halves(rank, grad_w_uv, uv_swapped, 1, min(kv_lora, 256))

        dcq_raw, dkv_raw = lax.optimization_barrier((draw[..., :q_lora], draw[..., q_lora:]))
        dcq_other, dkv_other = swap(dcq_raw), swap(dkv_raw)
        grad_hidden = (jnp.einsum('btq,dq->btd', dcq_raw, w_dq, preferred_element_type=F32) + jnp.einsum('btc,dc->btd', dkv_raw, w_dkv, preferred_element_type=F32)).astype(BF16)
        grad_w_dq, grad_w_dkv = down_wgrad(hidden, x_other, dcq_raw, dcq_other, dkv_raw, dkv_other)
        return (attn_out, grad_hidden, grad_w_dq, grad_g_q, grad_w_dkv, grad_g_kv, grad_w_uq, grad_w_uk, grad_w_uv, grad_w_o)

    seq_spec = P(None, 'cp', None)
    full_spec = P()
    head_spec = P(None, 'tp', None)
    out_head_spec = P('tp', None, None)
    all_specs = (seq_spec, seq_spec, full_spec, full_spec, full_spec, full_spec, head_spec, head_spec, head_spec, out_head_spec)
    return jax.shard_map(block, mesh=mesh, in_specs=all_specs, out_specs=all_specs, check_vma=False)
```
